32 devices in a mesh: zero: 8 (over z, y), width: 4 (over x, core).
Axes of the slice: x: 2, y: 2, z: 4, core: 2. Of those that a mesh axis runs over, the one named last changes fastest.
Arguments:
- train_query: float32 [7168, 7168], P('zero', 'width'), may hold values from -0.09375 to 0.09375
- slow_query: float32 [7168, 7168], P('zero', 'width'), may hold values from -0.0625 to 0.0625
- train_key: float32 [7168, 1024], P('zero', 'width'), may hold values from -0.09375 to 0.09375
- slow_key: float32 [7168, 1024], P('zero', 'width'), may hold values from -0.0625 to 0.0625
- train_value: float32 [7168, 1024], P('zero', 'width'), may hold values from -0.09375 to 0.09375
- slow_value: float32 [7168, 1024], P('zero', 'width'), may hold values from -0.0625 to 0.0625
- norm_train: float32 [7168], P(('zero', 'width')), may hold values from 0.25 to 1.75
- norm_step: float32 [7168], P(('zero', 'width')), may hold values from -0.3 to 0.3
Outputs:
- ready_query: bfloat16 [7168, 7168], P(None, 'width')
- ready_key: bfloat16 [7168, 1024], P(None, 'width')
- ready_value: bfloat16 [7168, 1024], P(None, 'width')
- scale_query: float32 [7168], P('width')
- scale_key: float32 [1024], P('width')
- scale_value: float32 [1024], P('width')
- serve_norm: bfloat16 [7168], replicated
- latest_query: float32 [7168, 7168], P('zero', 'width')
- latest_key: float32 [7168, 1024], P('zero', 'width')
- latest_value: float32 [7168, 1024], P('zero', 'width')
The draws below stay inside these ranges and needn't reach their ends.
All inputs are finite; a program needn't handle non-finite values.
Results may differ from the reference program's by a relative error of at most 0.0004.
Values may be sent and summed in bfloat16 or wider, within the bound.
A program may use at most 128 MiB of HBM per device.

```python
import jax
import jax.numpy as jnp
from jax import lax

D_MODEL = 7168
Q_DIM = 7168
KV_DIM = 1024


def strengthened(result, key, source, target, blocks, factor):
    def block_of(dim):
        return (jnp.arange(result.shape[dim]) // (result.shape[dim] // blocks)).reshape((-1,) + (1,) * (result.ndim - 1 - dim))

    near = jax.random.permutation(key, blocks)[block_of(target)]
    far = (block_of(target) + blocks // 2) % blocks
    return jnp.where((block_of(source) == near) | (block_of(source) == far), factor * result, result)


def levels(stream_key, extent, shards, smallest, high):
    def one(position, parts):
        heights = jax.random.uniform(jax.random.fold_in(jax.random.fold_in(stream_key, 6), position), (parts,), jnp.float32, smallest / len(shards), high / len(shards))
        return jnp.repeat(jnp.exp(heights), extent[position] // parts).reshape((-1,) + (1,) * (len(extent) - position - 1))

    factor_of = one(*shards[0])
    for cut in shards[1:]:
        factor_of = factor_of * one(*cut)
    return factor_of


def bell_draw(rng, extent, deviation, limit, shards=(), kind=jnp.bfloat16):
    entries = deviation * jax.random.normal(rng, extent, jnp.float32)
    if shards:
        entries = entries * levels(rng, extent, shards, -0.22, 0.18)
    return jnp.clip(entries, -limit, limit).astype(kind)


def noise_with(own_key, dims, deviation, bound, pieces, heavy, dtype=jnp.bfloat16):
    entries = deviation * jax.random.normal(own_key, dims, jnp.float32)
    if pieces:
        entries = entries * levels(own_key, dims, pieces, -0.22, 0.18)
    return jnp.clip(strengthened(entries, jax.random.fold_in(own_key, 3), *heavy), -bound, bound).astype(dtype)


def setup_inputs(seed: int = 0) -> dict:
    seeds = jax.random.split(jax.random.key(seed), 9)
    train_query = noise_with(seeds[0], (D_MODEL, Q_DIM), D_MODEL ** -0.5, 0.09375, ((0, 8), (1, 4)), (0, 1, 8, 2.0), jnp.float32)
    slow_query = bell_draw(seeds[1], (D_MODEL, Q_DIM), D_MODEL ** -0.5, 0.0625, ((0, 8), (1, 4)), jnp.float32)
    train_key = noise_with(seeds[2], (D_MODEL, KV_DIM), D_MODEL ** -0.5, 0.09375, ((0, 8), (1, 4)), (0, 1, 8, 2.0), jnp.float32)
    slow_key = bell_draw(seeds[3], (D_MODEL, KV_DIM), D_MODEL ** -0.5, 0.0625, ((0, 8), (1, 4)), jnp.float32)
    train_value = noise_with(seeds[4], (D_MODEL, KV_DIM), D_MODEL ** -0.5, 0.09375, ((0, 8), (1, 4)), (0, 1, 8, 2.0), jnp.float32)
    slow_value = bell_draw(seeds[5], (D_MODEL, KV_DIM), D_MODEL ** -0.5, 0.0625, ((0, 8), (1, 4)), jnp.float32)
    norm_train = jnp.clip(1.0 + 0.15 * jax.random.normal(seeds[6], (D_MODEL,), jnp.float32), 0.25, 1.75)
    norm_step = jnp.clip(jax.random.uniform(seeds[7], (D_MODEL,), jnp.float32, -0.3, 0.3) * levels(seeds[7], (D_MODEL,), ((0, 32),), -0.4, 0.0), -0.3, 0.3)
    return {"train_query": train_query, "slow_query": slow_query, "train_key": train_key, "slow_key": slow_key, "train_value": train_value, "slow_value": slow_value, "norm_train": norm_train, "norm_step": norm_step}


keep_rate = 0.5

def reference(train_query, slow_query, train_key, slow_key, train_value, slow_value, norm_train, norm_step):
    latest_query = keep_rate * slow_query + (1.0 - keep_rate) * train_query
    latest_key = keep_rate * slow_key + (1.0 - keep_rate) * train_key
    latest_value = keep_rate * slow_value + (1.0 - keep_rate) * train_value
    scale_query = jnp.sqrt(lax.optimization_barrier(jnp.sum(latest_query * latest_query, axis=0)))
    ready_query = (latest_query / scale_query).astype(jnp.bfloat16)
    scale_key = jnp.sqrt(lax.optimization_barrier(jnp.sum(latest_key * latest_key, axis=0)))
    ready_key = (latest_key / scale_key).astype(jnp.bfloat16)
    scale_value = jnp.sqrt(lax.optimization_barrier(jnp.sum(latest_value * latest_value, axis=0)))
    ready_value = (latest_value / scale_value).astype(jnp.bfloat16)
    serve_norm = (norm_train + norm_step).astype(jnp.bfloat16)
    return (ready_query, ready_key, ready_value, scale_query, scale_key, scale_value, serve_norm, latest_query, latest_key, latest_value)
```

```python
import functools

import jax
import jax.numpy as jnp
from jax import lax
from jax.experimental import pallas as pl
from jax.experimental.pallas import tpu as pltpu
from jax.sharding import PartitionSpec as P

keep_rate = 0.5
MESH = pl.DeviceIdType.MESH


def grid_of(count):
    fast = 1
    while (2 * fast) ** 2 <= count and count % (2 * fast) == 0:
        fast *= 2
    return count // fast, fast


def node_at(place, slow, fast):
    if fast == 1:
        return place
    deep = slow - 1
    back = place // (deep * fast)
    column = place // deep
    step = place % deep
    step = step + (column % 2) * (deep - 1 - 2 * step)
    z = (1 - back) * (1 + step)
    y = (1 - back) * column + back * (fast - 1 - (place - deep * fast))
    return z * fast + y


def place_of(node, slow, fast):
    if fast == 1:
        return node
    deep = slow - 1
    z, y = node // fast, node % fast
    out = (z + slow - 1) // slow
    step = z - 1
    step = step + (y % 2) * (deep - 1 - 2 * step)
    return out * (y * deep + step) + (1 - out) * (deep * fast + fast - 1 - y)


def average_kernel(tq, sq, tk, sk, tv, sv, lq, lk, lv, part):
    @pl.when(pl.program_id(0) == 0)
    def _():
        part[...] = jnp.zeros_like(part)

    at = 0
    for train, slow, latest in ((tq, sq, lq), (tk, sk, lk), (tv, sv, lv)):
        value = keep_rate * slow[...] + (1.0 - keep_rate) * train[...]
        latest[...] = value
        wide = value.shape[1]
        part[:, at : at + wide] += jnp.sum(value * value, axis=0, keepdims=True)
        at += wide


def average(arrays):
    rows = arrays[0].shape[0]
    tile = 112 if rows % 112 == 0 else 16
    wides = [a.shape[1] for a in arrays[::2]]

    def spec(wide):
        return pl.BlockSpec((tile, wide), lambda i: (i, 0))

    return pl.pallas_call(
        average_kernel,
        grid=(rows // tile,),
        in_specs=[spec(a.shape[1]) for a in arrays],
        out_specs=[spec(w) for w in wides] + [pl.BlockSpec((1, sum(wides)), lambda i: (0, 0))],
        out_shape=[jax.ShapeDtypeStruct((rows, w), jnp.float32) for w in wides]
        + [jax.ShapeDtypeStruct((1, sum(wides)), jnp.float32)],
        compiler_params=pltpu.CompilerParams(dimension_semantics=("arbitrary",)),
    )(*arrays)


def gather_kernel(
    count, across, cuts, wides, half,
    lq, lk, lv, part, norm_train, norm_step,
    rq, rk, rv, scale_q, scale_k, scale_v, norm_all,
    wq, wk, wv, nq, nk, nv, stats, scale,
    load_sem, keep_sem, stat_send, stat_recv, near_send, near_recv, far_send, far_recv,
    send_sem, recv_sem,
):
    me, side = lax.axis_index("zero"), lax.axis_index("width")
    slow, fast = grid_of(count)
    place = place_of(me, slow, fast)
    ahead = node_at(lax.rem(place + 1, count), slow, fast)
    behind = node_at(lax.rem(place + count - 1, count), slow, fast)
    rows = 2 * half
    latest, wide_in, narrow, ready = (lq, lk, lv), (wq, wk, wv), (nq, nk, nv), (rq, rk, rv)
    pieces = [(0, c * (half // cuts), half // cuts) for c in range(cuts)]
    pieces += [(1, 0, half), (2, 0, half)]

    loads = {}
    for i, (which, first, size) in enumerate(pieces):
        for way in range(2):
            at = pl.ds(way * half + first, size)
            loads[i, way] = pltpu.make_async_copy(
                latest[which].at[at], wide_in[which].at[at], load_sem.at[way, i]
            )
            loads[i, way].start()

    barrier = pltpu.get_barrier_semaphore()
    for k in range(1, count):
        pl.semaphore_signal(
            barrier, inc=1, device_id=(lax.rem(me + k, count), side), device_id_type=MESH
        )
    for k in range(1, across):
        pl.semaphore_signal(
            barrier, inc=1, device_id=(me, lax.rem(side + k, across)), device_id_type=MESH
        )
    stats[me] = part[...]
    mine = me * across + side
    norm_all[mine] = norm_train[...] + norm_step[...]
    pl.semaphore_wait(barrier, count + across - 2)

    def stat_copy(k):
        return pltpu.make_async_remote_copy(
            src_ref=stats.at[me], dst_ref=stats.at[me],
            send_sem=stat_send.at[k - 1], recv_sem=stat_recv.at[k - 1],
            device_id=(lax.rem(me + k, count), side), device_id_type=MESH,
        )

    def near_copy(k):
        return pltpu.make_async_remote_copy(
            src_ref=norm_all.at[mine], dst_ref=norm_all.at[mine],
            send_sem=near_send.at[k - 1], recv_sem=near_recv.at[k - 1],
            device_id=(me, lax.rem(side + k, across)), device_id_type=MESH,
        )

    def far_copy(k):
        at = pl.ds(me * across, across)
        return pltpu.make_async_remote_copy(
            src_ref=norm_all.at[at], dst_ref=norm_all.at[at],
            send_sem=far_send.at[k - 1], recv_sem=far_recv.at[k - 1],
            device_id=(lax.rem(me + k, count), side), device_id_type=MESH,
        )

    for k in range(1, count):
        stat_copy(k).start()
    for k in range(1, across):
        near_copy(k).start()
    for k in range(1, count):
        stat_copy(k).wait_recv()
    total = stats[0]
    for k in range(1, count):
        total = total + stats[k]
    scale[...] = jnp.sqrt(total)
    at = [0, wides[0], wides[0] + wides[1], sum(wides)]
    for i, out in enumerate((scale_q, scale_k, scale_v)):
        out[...] = scale[:, at[i] : at[i + 1]]

    def ring_copy(step, i, way):
        which, first, size = pieces[i]
        shift = step if way else count - step
        owner = node_at(lax.rem(place + shift, count), slow, fast)
        spot = pl.ds(pl.multiple_of(owner * rows + way * half + first, 16), size)
        if isinstance(step, int) and step == 0:
            source = narrow[which].at[pl.ds(way * half + first, size)]
        else:
            source = ready[which].at[spot]
        return pltpu.make_async_remote_copy(
            src_ref=source, dst_ref=ready[which].at[spot],
            send_sem=send_sem.at[way, step, i], recv_sem=recv_sem.at[way, step, i],
            device_id=(behind if way else ahead, side), device_id_type=MESH,
        )

    def arrival(step, i, way):
        which, first, size = pieces[i]
        shift = step + 1 if way else count - step - 1
        owner = node_at(lax.rem(place + shift, count), slow, fast)
        spot = pl.ds(pl.multiple_of(owner * rows + way * half + first, 16), size)
        return pltpu.make_async_remote_copy(
            src_ref=ready[which].at[spot], dst_ref=ready[which].at[spot],
            send_sem=send_sem.at[way, step, i], recv_sem=recv_sem.at[way, step, i],
            device_id=(behind if way else ahead, side), device_id_type=MESH,
        )

    keeps = []
    for i, (which, first, size) in enumerate(pieces):
        for way in range(2):
            spot = pl.ds(way * half + first, size)
            loads[i, way].wait()
            narrow[which][spot, :] = (
                wide_in[which][spot, :] / scale[:, at[which] : at[which + 1]]
            ).astype(jnp.bfloat16)
            ring_copy(0, i, way).start()
            home = pl.ds(pl.multiple_of(me * rows + way * half + first, 16), size)
            keep = pltpu.make_async_copy(
                narrow[which].at[spot], ready[which].at[home], keep_sem.at[way, i]
            )
            keep.start()
            keeps.append(keep)

    for k in range(1, across):
        near_copy(k).wait_recv()
    for k in range(1, count):
        far_copy(k).start()

    def forward(step, carry):
        for i in range(len(pieces)):
            for way in range(2):
                arrival(step - 1, i, way).wait_recv()
                ring_copy(step, i, way).start()
        return carry

    lax.fori_loop(1, count - 1, forward, 0)
    for i in range(len(pieces)):
        for way in range(2):
            arrival(count - 2, i, way).wait_recv()

    def drain(step, carry):
        for i in range(len(pieces)):
            for way in range(2):
                arrival(step, i, way).wait_send()
        return carry

    lax.fori_loop(0, count - 1, drain, 0)
    for keep in keeps:
        keep.wait()
    for k in range(1, count):
        stat_copy(k).wait_send()
        far_copy(k).wait()
    for k in range(1, across):
        near_copy(k).wait_send()


def gather(latest, part, norm_train, norm_step, count, across):
    rows = latest[0].shape[0]
    wides = [a.shape[1] for a in latest]
    half = rows // 2
    cuts = next(c for c in (4, 2, 1) if half % (16 * c) == 0)
    n = cuts + 2
    piece = norm_train.shape[0]
    hbm = pl.BlockSpec(memory_space=pl.ANY)
    vmem = pl.BlockSpec(memory_space=pltpu.VMEM)
    dma = pltpu.SemaphoreType.DMA
    outs = pl.pallas_call(
        functools.partial(gather_kernel, count, across, cuts, wides, half),
        in_specs=[hbm] * 3 + [vmem] * 3,
        out_specs=[hbm] * 3 + [vmem] * 4,
        out_shape=[jax.ShapeDtypeStruct((count * rows, w), jnp.bfloat16) for w in wides]
        + [jax.ShapeDtypeStruct((1, w), jnp.float32) for w in wides]
        + [jax.ShapeDtypeStruct((count * across, 1, piece), jnp.float32)],
        scratch_shapes=[pltpu.VMEM((rows, w), jnp.float32) for w in wides]
        + [pltpu.VMEM((rows, w), jnp.bfloat16) for w in wides]
        + [
            pltpu.VMEM((count, 1, sum(wides)), jnp.float32),
            pltpu.VMEM((1, sum(wides)), jnp.float32),
            dma((2, n)),
            dma((2, n)),
            dma((count - 1,)),
            dma((count - 1,)),
            dma((across - 1,)),
            dma((across - 1,)),
            dma((count - 1,)),
            dma((count - 1,)),
            dma((2, count - 1, n)),
            dma((2, count - 1, n)),
        ],
        compiler_params=pltpu.CompilerParams(collective_id=0, has_side_effects=True),
    )(*latest, part, norm_train.reshape(1, piece), norm_step.reshape(1, piece))
    return outs


def solution(mesh):
    count, across = mesh.shape["zero"], mesh.shape["width"]

    def body(
        train_query, slow_query, train_key, slow_key, train_value, slow_value, norm_train, norm_step
    ):
        *latest, part = average(
            (train_query, slow_query, train_key, slow_key, train_value, slow_value)
        )
        rq, rk, rv, sq, sk, sv, norm = gather(latest, part, norm_train, norm_step, count, across)
        serve_norm = norm.astype(jnp.bfloat16).reshape(-1)
        return (rq, rk, rv, sq.reshape(-1), sk.reshape(-1), sv.reshape(-1), serve_norm, *latest)

    in_specs = (P("zero", "width"),) * 6 + (P(("zero", "width")),) * 2
    out_specs = (
        (P(None, "width"),) * 3 + (P("width"),) * 3 + (P(),) + (P("zero", "width"),) * 3
    )
    return jax.shard_map(body, mesh=mesh, in_specs=in_specs, out_specs=out_specs, check_vma=False)
```

```python
import functools

import jax
import jax.numpy as jnp
from jax import lax
from jax.experimental import pallas as pl
from jax.experimental.pallas import tpu as pltpu
from jax.sharding import PartitionSpec as P

keep_rate = 0.5
MESH = pl.DeviceIdType.MESH


def grid_of(count):
    fast = 1
    while (2 * fast) ** 2 <= count and count % (2 * fast) == 0:
        fast *= 2
    return count // fast, fast


def node_at(place, slow, fast):
    if fast == 1:
        return place
    deep = slow - 1
    back = place // (deep * fast)
    column = place // deep
    step = place % deep
    step = step + (column % 2) * (deep - 1 - 2 * step)
    z = (1 - back) * (1 + step)
    y = (1 - back) * column + back * (fast - 1 - (place - deep * fast))
    return z * fast + y


def place_of(node, slow, fast):
    if fast == 1:
        return node
    deep = slow - 1
    z, y = node // fast, node % fast
    out = (z + slow - 1) // slow
    step = z - 1
    step = step + (y % 2) * (deep - 1 - 2 * step)
    return out * (y * deep + step) + (1 - out) * (deep * fast + fast - 1 - y)


def gather_kernel(
    count, across, width, half, tile,
    tq, sq, tk, sk, tv, sv, norm_train, norm_step,
    rq, rk, rv, lq, lk, lv, scale_q, scale_k, scale_v, norm_all,
    itq, isq, itk, isk, itv, isv, stats_a, stats_b,
    load_sem, stat_send, stat_recv, near_send, near_recv, far_send, far_recv,
    send_sem, recv_sem,
):
    me, side = lax.axis_index("zero"), lax.axis_index("width")
    slow, fast = grid_of(count)
    place = place_of(me, slow, fast)
    ahead = node_at(lax.rem(place + 1, count), slow, fast)
    behind = node_at(lax.rem(place + count - 1, count), slow, fast)
    rows = 2 * half
    trains, slows = ((tq, itq), (tk, itk), (tv, itv)), ((sq, isq), (sk, isk), (sv, isv))
    latest, ready, scales = (lq, lk, lv), (rq, rk, rv), (scale_q, scale_k, scale_v)
    groups = [(1, 0), (2, 0)] + [(0, c) for c in range(tq.shape[1] // width)]

    def columns(c):
        return pl.ds(c * width, width)

    loads = []
    for i, (which, c) in enumerate(groups):
        pair = []
        for j, arrays in enumerate((trains, slows)):
            far, near = arrays[which]
            pair.append(
                pltpu.make_async_copy(far.at[:, columns(c)], near.at[:, columns(c)], load_sem.at[j, i])
            )
            pair[-1].start()
        loads.append(pair)

    barrier = pltpu.get_barrier_semaphore()
    for k in range(1, count):
        pl.semaphore_signal(
            barrier, inc=1, device_id=(lax.rem(me + k, count), side), device_id_type=MESH
        )
    for k in range(1, across):
        pl.semaphore_signal(
            barrier, inc=1, device_id=(me, lax.rem(side + k, across)), device_id_type=MESH
        )
    mine = me * across + side
    norm_all[mine] = norm_train[...] + norm_step[...]

    def stat_copy(part, k):
        stats = (stats_a, stats_b)[part]
        return pltpu.make_async_remote_copy(
            src_ref=stats.at[me], dst_ref=stats.at[me],
            send_sem=stat_send.at[part, k - 1], recv_sem=stat_recv.at[part, k - 1],
            device_id=(lax.rem(me + k, count), side), device_id_type=MESH,
        )

    def near_copy(k):
        return pltpu.make_async_remote_copy(
            src_ref=norm_all.at[mine], dst_ref=norm_all.at[mine],
            send_sem=near_send.at[k - 1], recv_sem=near_recv.at[k - 1],
            device_id=(me, lax.rem(side + k, across)), device_id_type=MESH,
        )

    def far_copy(k):
        at = pl.ds(me * across, across)
        return pltpu.make_async_remote_copy(
            src_ref=norm_all.at[at], dst_ref=norm_all.at[at],
            send_sem=far_send.at[k - 1], recv_sem=far_recv.at[k - 1],
            device_id=(lax.rem(me + k, count), side), device_id_type=MESH,
        )

    def average(i, stats, c_out):
        which, c = groups[i]
        for load in loads[i]:
            load.wait()

        def step(t, total):
            at = pl.ds(pl.multiple_of(t * tile, 16), tile)
            value = (
                keep_rate * slows[which][1][at, columns(c)]
                + (1.0 - keep_rate) * trains[which][1][at, columns(c)]
            )
            latest[which][at, columns(c)] = value
            return total + jnp.sum((value * value).reshape(tile // 8, 8, width), axis=0)

        total = lax.fori_loop(0, rows // tile, step, jnp.zeros((8, width), jnp.float32))
        stats[me, :, columns(c_out)] = jnp.sum(total, axis=0, keepdims=True)

    def ring_copy(owner, step, i, way):
        which, c = groups[i]
        spot = pl.ds(pl.multiple_of(owner * rows + way * half, 16), half)
        piece = ready[which].at[spot, columns(c)]
        return pltpu.make_async_remote_copy(
            src_ref=piece, dst_ref=piece,
            send_sem=send_sem.at[way, step, i], recv_sem=recv_sem.at[way, step, i],
            device_id=(behind if way else ahead, side), device_id_type=MESH,
        )

    def owner_of(step, way):
        return node_at(lax.rem(place + (step if way else count - step), count), slow, fast)

    def send_own(i):
        which, c = groups[i]
        scale = scales[which][:, columns(c)]
        for way in range(2):

            def step(t, carry):
                at = pl.multiple_of(way * half + t * tile, 16)
                home = pl.multiple_of(me * rows + at, 16)
                ready[which][pl.ds(home, tile), columns(c)] = (
                    latest[which][pl.ds(at, tile), columns(c)] / scale
                ).astype(jnp.bfloat16)
                return carry

            lax.fori_loop(0, half // tile, step, 0)
            ring_copy(me, 0, i, way).start()

    def finish(part, members):
        stats = (stats_a, stats_b)[part]
        for k in range(1, count):
            stat_copy(part, k).wait_recv()
        total = stats[0]
        for k in range(1, count):
            total = total + stats[k]
        total = jnp.sqrt(total)
        at = 0
        for which in members:
            wide = scales[which].shape[1]
            scales[which][...] = total[:, at : at + wide]
            at += wide

    average(0, stats_a, 0)
    average(1, stats_a, 1)
    pl.semaphore_wait(barrier, count + across - 2)
    for k in range(1, count):
        stat_copy(0, k).start()
    for k in range(1, across):
        near_copy(k).start()
    early = 2 + (len(groups) - 2) // 2 + 1
    for i in range(2, early):
        average(i, stats_b, groups[i][1])
    finish(0, (1, 2))
    send_own(0)
    send_own(1)
    for i in range(early, len(groups)):
        average(i, stats_b, groups[i][1])
    for k in range(1, count):
        stat_copy(1, k).start()
    finish(1, (0,))
    for i in range(2, len(groups)):
        send_own(i)
    for k in range(1, across):
        near_copy(k).wait_recv()
    for k in range(1, count):
        far_copy(k).start()

    def forward(step, carry):
        owners = owner_of(step, 0), owner_of(step, 1)
        for i in range(len(groups)):
            for way in range(2):
                ring_copy(owners[way], step - 1, i, way).wait_recv()
                ring_copy(owners[way], step, i, way).start()
        return carry

    lax.fori_loop(1, count - 1, forward, 0)
    for i in range(len(groups)):
        for way in range(2):
            ring_copy(owner_of(count - 1, way), count - 2, i, way).wait_recv()

    def drain(step, carry):
        for i in range(len(groups)):
            for way in range(2):
                ring_copy(owner_of(step, way), step, i, way).wait_send()
        return carry

    lax.fori_loop(0, count - 1, drain, 0)
    for k in range(1, count):
        stat_copy(0, k).wait_send()
        stat_copy(1, k).wait_send()
        far_copy(k).wait()
    for k in range(1, across):
        near_copy(k).wait_send()


def gather(arrays, norm_train, norm_step, count, across):
    rows = arrays[0].shape[0]
    wides = [a.shape[1] for a in arrays[::2]]
    half = rows // 2
    width = wides[1]
    tile = 112 if half % 112 == 0 else 16
    n = sum(wides) // width
    piece = norm_train.shape[0]
    hbm = pl.BlockSpec(memory_space=pl.ANY)
    vmem = pl.BlockSpec(memory_space=pltpu.VMEM)
    dma = pltpu.SemaphoreType.DMA
    return pl.pallas_call(
        functools.partial(gather_kernel, count, across, width, half, tile),
        in_specs=[hbm] * 6 + [vmem] * 2,
        out_specs=[vmem] * 10,
        out_shape=[pltpu.VMEM((count * rows, w), jnp.bfloat16) for w in wides]
        + [pltpu.VMEM((rows, w), jnp.float32) for w in wides]
        + [pltpu.VMEM((1, w), jnp.float32) for w in wides]
        + [jax.ShapeDtypeStruct((count * across, 1, piece), jnp.float32)],
        scratch_shapes=[pltpu.VMEM(a.shape, jnp.float32) for a in arrays]
        + [
            pltpu.VMEM((count, 1, 2 * width), jnp.float32),
            pltpu.VMEM((count, 1, wides[0]), jnp.float32),
            dma((2, n)),
            dma((2, count - 1)),
            dma((2, count - 1)),
            dma((across - 1,)),
            dma((across - 1,)),
            dma((count - 1,)),
            dma((count - 1,)),
            dma((2, count - 1, n)),
            dma((2, count - 1, n)),
        ],
        compiler_params=pltpu.CompilerParams(
            collective_id=0, has_side_effects=True,
            vmem_limit_bytes=4 * sum(a.size for a in arrays) + 2**21,
        ),
    )(*arrays, norm_train.reshape(1, piece), norm_step.reshape(1, piece))


def store_kernel(cuts, count, *refs):
    wide, thin = count, (len(refs) - 1) // 2 - count
    wide_in, scale_in = refs[:wide], refs[wide : wide + thin]
    wide_out, scale_out = refs[wide + thin : 2 * wide + thin], refs[2 * wide + thin : -1]
    sem = refs[-1]
    copies = []
    for i, (source, target) in enumerate(zip(wide_in, wide_out)):
        size = source.shape[0] // cuts
        for c in range(cuts):
            at = pl.ds(c * size, size)
            copies.append(pltpu.make_async_copy(source.at[at], target.at[at], sem.at[i, c]))
            copies[-1].start()
    for source, target in zip(scale_in, scale_out):
        target[...] = source[0, :]
    for copy in copies:
        copy.wait()


def store(arrays, scales):
    cuts = 8
    hbm = pl.BlockSpec(memory_space=pl.ANY)
    vmem = pl.BlockSpec(memory_space=pltpu.VMEM)
    return pl.pallas_call(
        functools.partial(store_kernel, cuts, len(arrays)),
        in_specs=[vmem] * (len(arrays) + len(scales)),
        out_specs=[hbm] * len(arrays) + [vmem] * len(scales),
        out_shape=[jax.ShapeDtypeStruct(a.shape, a.dtype) for a in arrays]
        + [jax.ShapeDtypeStruct((s.shape[1],), s.dtype) for s in scales],
        scratch_shapes=[pltpu.SemaphoreType.DMA((len(arrays), cuts))],
        compiler_params=pltpu.CompilerParams(vmem_limit_bytes=2**20),
    )(*arrays, *scales)


def solution(mesh):
    count, across = mesh.shape["zero"], mesh.shape["width"]

    def body(
        train_query, slow_query, train_key, slow_key, train_value, slow_value, norm_train, norm_step
    ):
        *arrays, norm = gather(
            (train_query, slow_query, train_key, slow_key, train_value, slow_value),
            norm_train, norm_step, count, across,
        )
        outs = store(arrays[:1], ()) + store(arrays[1:6], arrays[6:])
        serve_norm = norm.astype(jnp.bfloat16).reshape(-1)
        return (*outs[:3], *outs[6:], serve_norm, *outs[3:6])

    in_specs = (P("zero", "width"),) * 6 + (P(("zero", "width")),) * 2
    out_specs = (
        (P(None, "width"),) * 3 + (P("width"),) * 3 + (P(),) + (P("zero", "width"),) * 3
    )
    return jax.shard_map(body, mesh=mesh, in_specs=in_specs, out_specs=out_specs, check_vma=False)
```
